32 devices in a mesh: sub: 4 (over y, x), elem: 8 (over z, core).
Axes of the slice: x: 2, y: 2, z: 4, core: 2. Of those that a mesh axis runs over, the one named last changes fastest.
Arguments:
- element_tiles: bfloat16 [256, 128, 128], P(('sub', 'elem')), parts along dimension 0, may hold values from -0.5 to 0.5
- element_blocks: int32 [256, 2], P(('sub', 'elem')), parts along dimension 0, may hold values from 0 to 31
- mode_shapes: bfloat16 [16384, 1024], P(('sub', 'elem')), parts along dimension 0, may hold values from -0.5 to 0.5
- trial_modes: bfloat16 [4096, 128], P('sub'), parts along dimension 0, may hold values from -0.1875 to 0.1875
Outputs:
- reduced_stiffness: float32 [4096, 1024], P(('sub', 'elem')), parts along dimension 0
- interface_forces: float32 [4096, 128], P(('sub', 'elem')), parts along dimension 0
The draws below stay inside these ranges and needn't reach their ends.
There are 4 independent parts, one for each index of `sub`. The reference program is written for one: setup_inputs(seed, part) draws one part's arguments, and reference() takes and returns one part's arrays. A program takes and returns all parts, laid end to end along the dimension named above; each array names one. Nothing has to cross between parts.
Inputs may be any that keep to these rules, and one draw needn't show every extreme that they name: `element_blocks`: each row gives the row block and the column block of one element tile.
All inputs are finite; a program needn't handle non-finite values.
Results may differ from the reference program's by a relative error of at most 0.0029.
Values may be sent and summed in bfloat16 or wider, within the bound.
No kernel may reach another device: no remote copies, remote signals or barrier semaphores. Data moves between devices by JAX's collectives and lax.ppermute only.
A program may use at most 64 MiB of HBM per device.

```python
import jax
import jax.numpy as jnp
from jax import lax

NI = 4096
M = 1024
BLOCK = 128
NRHS = 128
ELEMS = 64
NB = 32


def place_ends(result, key, low, largest):
    spot = [jax.random.randint(jax.random.fold_in(key, axis), (), 0, length) for axis, length in enumerate(result.shape)]
    main_axis = result.shape.index(max(result.shape))
    beside = spot[:main_axis] + [(spot[main_axis] + 1) % result.shape[main_axis]] + spot[main_axis + 1:]
    return result.at[tuple(spot)].set(low).at[tuple(beside)].set(largest)


def block_levels(stream_key, dims, cuts, low, high):
    def one(dim, parts):
        draws = jax.random.uniform(jax.random.fold_in(jax.random.fold_in(stream_key, 6), dim), (parts,), jnp.float32, low / len(cuts), high / len(cuts))
        return jnp.repeat(jnp.exp(draws), dims[dim] // parts).reshape((-1,) + (1,) * (len(dims) - dim - 1))

    level = one(*cuts[0])
    for cut in cuts[1:]:
        level = level * one(*cut)
    return level


def centred(rng, dims, width, bound, cuts=(), kind=jnp.bfloat16):
    level = block_levels(rng, dims, cuts, -0.22, 0.18) if cuts else 1.0
    result = jax.random.normal(rng, dims, jnp.float32) * width * level
    return jnp.minimum(jnp.maximum(result, -bound), bound).astype(kind)


def setup_inputs(seed: int = 0, part: int = 0) -> dict:
    key_of = jax.random.split(jax.random.key(seed), 5)
    own_keys = jax.random.split(jax.random.fold_in(key_of[4], part), 5)
    return {
        "element_tiles": centred(own_keys[0], (ELEMS, BLOCK, BLOCK), BLOCK ** -0.5, 0.5, ((0, 8),)),
        "element_blocks": place_ends(jax.random.randint(own_keys[1], (ELEMS, 2), 0, NB), jax.random.fold_in(own_keys[1], 1), 0, NB - 1).astype(jnp.int32),
        "mode_shapes": centred(own_keys[2], (NI, M), BLOCK ** -0.5, 0.5, ((0, 8),)),
        "trial_modes": centred(own_keys[3], (M, NRHS), M ** -0.5, 0.1875),
    }


def reference(element_tiles, element_blocks, mode_shapes, trial_modes):
    blocks = mode_shapes.reshape(NI // BLOCK, BLOCK, M)
    row_side = jnp.take(blocks, element_blocks[:, 0], axis=0).reshape(-1, M)
    col_side = jnp.take(blocks, element_blocks[:, 1], axis=0)
    stiff_modes = jnp.einsum("eij,ejm->eim", element_tiles.astype(jnp.float32), col_side.astype(jnp.float32))
    stiff_modes = stiff_modes.astype(jnp.bfloat16).reshape(-1, M)
    reduced = lax.dot_general(row_side, stiff_modes, (((0,), (0,)), ((), ())), preferred_element_type=jnp.float32)
    forces = jnp.dot(reduced, trial_modes.astype(jnp.float32), precision=lax.Precision.HIGHEST)
    return reduced, forces
```

```python
import functools

import jax
import jax.numpy as jnp
from jax import lax
from jax.experimental import pallas as pl
from jax.experimental.pallas import tpu as pltpu
from jax.sharding import PartitionSpec as P

AXES = ("sub", "elem")


class Plan:
    def __init__(self, mesh):
        self.parts, self.places = mesh.shape["sub"], mesh.shape["elem"]
        self.chips = self.places // 2
        self.root = self.chips // 2 - 1

    def kind(self, part):
        return (part ^ (part >> 1)) & 1

    def chip(self, part, step):
        return self.chips - 1 - step if self.kind(part) else step

    def device(self, part, step, core):
        return part * self.places + self.chip(part, step) * 2 + core

    def pairs(self, route):
        return [
            route(part, core) for part in range(self.parts) for core in range(2)
        ]

    def to_root(self, step):
        return self.pairs(lambda p, c: (self.device(p, step, c), self.device(p, self.root, c)))

    def to_side(self, step, flip):
        def route(p, c):
            here = self.device(p, step, c)
            return here, here + ((p ^ flip) - p) * self.places

        return self.pairs(route)

    def side_to_root(self, step, flip):
        def route(p, c):
            here = self.device(p, step, c)
            return here + ((p ^ flip) - p) * self.places, self.device(p, self.root, c)

        return self.pairs(route)

    def swap(self):
        return self.pairs(lambda p, c: (self.device(p, self.root, c), self.device(p, self.root, 1 - c)))

    def from_root(self, step, cross):
        return self.pairs(lambda p, c: (self.device(p, self.root, c), self.device(p, step, c ^ cross)))


def root_kernel(layout, blocks_ref, where_ref, *refs):
    chips, per, width, modes, elems = layout
    half = modes // 2
    n_p, n_t = 2 * chips + 2, 2 * chips
    p_in, t_in = refs[:n_p], refs[n_p : n_p + n_t]
    out_ref = refs[n_p + n_t]
    p_all, t_all, q_sum, q_low, k_acc, sems = refs[n_p + n_t + 1 :]
    kind, core = where_ref[0], where_ref[1]
    depth = per * width
    local = elems // (2 * chips)

    copies = []
    row = 0
    for i, ref in enumerate(p_in):
        rows = ref.shape[0]
        copies.append(pltpu.make_async_copy(ref, p_all.at[pl.ds(row, rows), :], sems.at[i]))
        row += rows
    for i, ref in enumerate(t_in):
        copies.append(pltpu.make_async_copy(ref, t_all.at[pl.ds(i * local, local)], sems.at[n_p + i]))
    for copy in copies:
        copy.start()
    q_sum[...] = jnp.zeros_like(q_sum)
    for copy in copies:
        copy.wait()

    def slot(block):
        place = block // per
        chip, k = place // 2, place % 2
        step = jnp.where(kind == 1, chips - 1 - chip, chip)
        return (step * 2 + (k ^ core)) * per + block % per

    columns = pl.ds(pl.multiple_of(core * half, half), half)

    def element(e, carry):
        place, t = e // local, e % local
        chip, k = place // 2, place % 2
        step = jnp.where(kind == 1, chips - 1 - chip, chip)
        tile = (step * 2 + (k ^ core)) * local + t
        r, c = slot(blocks_ref[e, 0]), slot(blocks_ref[e, 1])
        col = p_all[pl.ds(pl.multiple_of(c * width, width), width), columns]
        stiff = jnp.dot(t_all[tile], col, preferred_element_type=jnp.float32).astype(jnp.bfloat16)
        rows = pl.ds(pl.multiple_of(r * width, width), width)
        q_sum[rows, :] += stiff.astype(jnp.float32)
        return carry

    lax.fori_loop(0, elems, element, 0)

    k_acc[...] = jnp.zeros_like(k_acc)
    chunk = 4 * width

    def contract(i, carry):
        rows = pl.ds(pl.multiple_of(i * chunk, chunk), chunk)
        q_low[rows, :] = q_sum[rows, :].astype(jnp.bfloat16)
        k_acc[...] += lax.dot_general(
            p_all[rows, :], q_low[rows, :], (((0,), (0,)), ((), ())), preferred_element_type=jnp.float32
        )
        return carry

    lax.fori_loop(0, depth * 2 * chips // chunk, contract, 0)
    strip = modes // (2 * chips)
    for step in range(chips):
        chip = jnp.where(kind == 1, chips - 1 - step, step)
        for cross in range(2):
            first = pl.multiple_of((chip * 2 + (core ^ cross)) * strip, strip)
            out_ref[cross, step] = k_acc[pl.ds(first, strip), :].astype(jnp.bfloat16)


def final_kernel(steps, where_ref, trial_ref, *refs):
    n = len(steps)
    same, cross = refs[:n], refs[n : 2 * n]
    k_ref, f_ref, rows = refs[2 * n :]
    step, core = where_ref[0], where_ref[1]
    half = same[0].shape[1]
    mine = pl.ds(pl.multiple_of(core * half, half), half)
    other = pl.ds(pl.multiple_of((1 - core) * half, half), half)
    for i, at in enumerate(steps):

        @pl.when(step == at)
        def _():
            rows[:, mine] = same[i][...]
            rows[:, other] = cross[i][...]

    k = rows[...]
    k_ref[...] = k.astype(jnp.float32)
    f_ref[...] = jnp.dot(k, trial_ref[...], preferred_element_type=jnp.float32)


def body(plan, element_tiles, element_blocks, mode_shapes, trial_modes):
    part, place = lax.axis_index("sub"), lax.axis_index("elem")
    kind = (part ^ (part >> 1)) & 1
    core = place % 2
    chip = place // 2
    step = jnp.where(kind == 1, plan.chips - 1 - chip, chip)
    local, width, _ = element_tiles.shape
    depth, modes = mode_shapes.shape
    root, chips = plan.root, plan.chips

    def send(x, pairs):
        return lax.ppermute(x, AXES, pairs)

    near = root + 1
    cut = depth // 2
    side_x = send(mode_shapes[:cut], plan.to_side(near, 1))
    side_y = send(mode_shapes[cut:], plan.to_side(near, 2))
    p_at, t_at = {root: mode_shapes}, {root: element_tiles}
    for s in range(chips - 1, -1, -1):
        if s == root:
            continue
        t_at[s] = send(element_tiles, plan.to_root(s))
        if s != near:
            p_at[s] = send(mode_shapes, plan.to_root(s))
    p_x = send(side_x, plan.side_to_root(near, 1))
    p_y = send(side_y, plan.side_to_root(near, 2))
    blocks = lax.all_gather(element_blocks, "elem", axis=0, tiled=True)

    p_in, t_in = [], []
    for s in range(chips):
        if s == near:
            p_in += [p_x, p_y, send(p_x, plan.swap()), send(p_y, plan.swap())]
        else:
            p_in += [p_at[s], send(p_at[s], plan.swap())]
        t_in += [t_at[s], send(t_at[s], plan.swap())]

    elems = local * plan.places
    layout = (chips, depth // width, width, modes, elems)
    strip = modes // plan.places
    half = modes // 2
    any_spec = pl.BlockSpec(memory_space=pl.ANY)
    smem = pl.BlockSpec(memory_space=pltpu.SMEM)
    vmem = pl.BlockSpec(memory_space=pltpu.VMEM)
    pieces = pl.pallas_call(
        functools.partial(root_kernel, layout),
        out_shape=jax.ShapeDtypeStruct((2, chips, strip, half), jnp.bfloat16),
        in_specs=[smem, smem] + [any_spec] * (len(p_in) + len(t_in)),
        out_specs=vmem,
        scratch_shapes=[
            pltpu.VMEM((depth * plan.places, modes), jnp.bfloat16),
            pltpu.VMEM((elems, width, width), jnp.bfloat16),
            pltpu.VMEM((depth * plan.places, half), jnp.float32),
            pltpu.VMEM((depth * plan.places, half), jnp.bfloat16),
            pltpu.VMEM((modes, half), jnp.float32),
            pltpu.SemaphoreType.DMA((len(p_in) + len(t_in),)),
        ],
        name="root_project",
    )(blocks, jnp.stack([kind, core]).astype(jnp.int32), *p_in, *t_in)

    order = sorted(range(chips), key=lambda s: -abs(s - root))
    same, cross = [], []
    for s in order:
        same.append(pieces[0, s] if s == root else send(pieces[0, s], plan.from_root(s, 0)))
        cross.append(send(pieces[1, s], plan.from_root(s, 1)))
    return pl.pallas_call(
        functools.partial(final_kernel, order),
        out_shape=(
            jax.ShapeDtypeStruct((strip, modes), jnp.float32),
            jax.ShapeDtypeStruct((strip, trial_modes.shape[1]), jnp.float32),
        ),
        in_specs=[smem, vmem] + [vmem] * (2 * chips),
        out_specs=(vmem, vmem),
        scratch_shapes=[pltpu.VMEM((strip, modes), jnp.bfloat16)],
        name="rows_and_forces",
    )(jnp.stack([step, core]).astype(jnp.int32), trial_modes, *same, *cross)


def solution(mesh):
    in_specs = (
        P(AXES, None, None),
        P(AXES, None),
        P(AXES, None),
        P("sub", None),
    )
    out_specs = (P(AXES, None), P(AXES, None))
    return jax.shard_map(
        functools.partial(body, Plan(mesh)), mesh=mesh, in_specs=in_specs, out_specs=out_specs, check_vma=False
    )
```

```python
import functools

import jax
import jax.numpy as jnp
from jax import lax
from jax.experimental import pallas as pl
from jax.experimental.pallas import tpu as pltpu
from jax.sharding import PartitionSpec as P


AXES = ("sub", "elem")
LANES, BELOW = 128, 8
SPARE = 3 << 20
SMEM = pl.BlockSpec(memory_space=pltpu.SMEM)
VMEM = pl.BlockSpec(memory_space=pltpu.VMEM)
ANY = pl.BlockSpec(memory_space=pl.ANY)
HBM = pl.BlockSpec(memory_space=pltpu.HBM)


class Plan:
    def __init__(self, mesh):
        self.parts, self.places = mesh.shape["sub"], mesh.shape["elem"]
        self.chips = self.places // 2
        self.root = self.chips // 2 - 1
        self.beyond = self.root + 1
        self.paired = self.parts % 4 == 0
        self.flips = (1, 2) if self.paired else ()

    def kind(self, part):
        return (part ^ (part >> 1)) & 1 if self.paired else part * 0

    def device(self, part, step, core):
        chip = self.chips - 1 - step if self.kind(part) else step
        return part * self.places + chip * 2 + core

    def beside(self, part, step, core, flip):
        return self.device(part, step, core) + ((part ^ flip) - part) * self.places

    def pairs(self, route):
        return [route(part, core) for part in range(self.parts) for core in range(2)]

    def to_root(self, step):
        return self.pairs(lambda p, c: (self.device(p, step, c), self.device(p, self.root, c)))

    def aside(self, step, flip):
        return self.pairs(lambda p, c: (self.device(p, step, c), self.beside(p, step, c, flip)))

    def aside_to_root(self, step, flip):
        return self.pairs(lambda p, c: (self.beside(p, step, c, flip), self.device(p, self.root, c)))

    def swap(self):
        return self.pairs(lambda p, c: (self.device(p, self.root, c), self.device(p, self.root, 1 - c)))

    def from_root(self, step, cross):
        return self.pairs(lambda p, c: (self.device(p, self.root, c), self.device(p, step, c ^ cross)))


def pack_kernel(cuts, p_ref, t_ref, b_ref, all_ref, *rest):
    parts, low_ref, sems = rest[:-2], rest[-2], rest[-1]
    depth, modes = p_ref.shape
    local, width, _ = t_ref.shape
    per = depth // width
    copies = [pltpu.make_async_copy(p_ref, all_ref.at[pl.ds(0, depth), pl.ds(0, modes)], sems.at[local])]
    for t in range(local):
        row, column = t % per * width, modes + t // per * width
        copies.append(
            pltpu.make_async_copy(t_ref.at[t], all_ref.at[pl.ds(row, width), pl.ds(column, width)], sems.at[t])
        )
    for copy in copies:
        copy.start()
    low_ref[...] = jnp.zeros_like(low_ref)
    low_ref[: b_ref.shape[0], :local] = b_ref[...]
    all_ref[depth:, :] = jnp.zeros((BELOW, all_ref.shape[1]), all_ref.dtype)
    all_ref[depth:, :LANES] = low_ref[...].astype(jnp.float32).astype(all_ref.dtype)
    for copy in copies:
        copy.wait()
    for i, part in enumerate(parts):
        low, high = cuts[i], cuts[i + 1]
        part[: high - low, :] = all_ref[low:high, :]
        if part.shape[0] > high - low:
            part[high - low :, :] = all_ref[depth:, :]


def join_kernel(cuts, *refs):
    parts, all_ref = refs[:-1], refs[-1]
    for part, low, high in zip(parts, cuts[:-1], cuts[1:]):
        all_ref[low:high, :] = part[: high - low, :]
        if part.shape[0] > high - low:
            all_ref[cuts[-1] :, :] = part[high - low :, :]


def root_kernel(plan, spans, width, modes, elems, where_ref, *refs):
    chips, n, half, below = plan.chips, len(spans), modes // 2, BELOW
    p_in, outs = refs[:n], refs[n : n + 2 * chips]
    p_all, t_all, low_idx, vec_idx, idx, q_sum, q_low, k_acc, sems = refs[n + 2 * chips :]
    kind, core = where_ref[0], where_ref[1]
    depth, local = p_all.shape[0] // plan.places, elems // plan.places
    per = depth // width
    mine = pl.ds(pl.multiple_of(core * half, half), half)
    rest = pl.ds(pl.multiple_of((1 - core) * half, half), half)

    first, second, numbers = [], [], []
    for i, (row, rows) in enumerate(spans):
        src, to = pl.ds(0, rows), pl.ds(row, rows)
        if p_in[i].shape[0] > rows:
            slot = row // depth
            numbers.append(
                pltpu.make_async_copy(
                    p_in[i].at[pl.ds(rows, below), pl.ds(0, LANES)],
                    low_idx.at[pl.ds(slot * below, below), :],
                    sems.at[3 * n + i],
                )
            )
        first.append(
            pltpu.make_async_copy(p_in[i].at[src, pl.ds(modes, t_all.shape[1])], t_all.at[to, :], sems.at[n + i])
        )
        first.append(pltpu.make_async_copy(p_in[i].at[src, mine], p_all.at[to, mine], sems.at[i]))
        second.append(pltpu.make_async_copy(p_in[i].at[src, rest], p_all.at[to, rest], sems.at[2 * n + i]))
    for copy in numbers + first + second:
        copy.start()
    for copy in numbers:
        copy.wait()
    vec_idx[...] = low_idx[...].astype(jnp.float32).astype(jnp.int32)
    to_smem = pltpu.make_async_copy(vec_idx, idx, sems.at[4 * n])
    to_smem.start()
    q_sum[...] = jnp.zeros_like(q_sum)
    to_smem.wait()
    for copy in first:
        copy.wait()

    def row_of(block):
        place, b = block // per, block % per
        chip, other = place // 2, (place % 2) ^ core
        step = jnp.where(kind == 1, chips - 1 - chip, chip)
        return pl.ds(pl.multiple_of(((step * 2 + other) * per + b) * width, width), width)

    def element(e, carry):
        slot, t = e // local, e % local
        tile = t_all[
            pl.ds(pl.multiple_of(slot * depth + t % per * width, width), width),
            pl.ds(pl.multiple_of(t // per * width, width), width),
        ]
        r, c = idx[slot * below, t], idx[slot * below + 1, t]
        stiff = jnp.dot(tile, p_all[row_of(c), mine], preferred_element_type=jnp.float32).astype(jnp.bfloat16)
        q_sum[row_of(r), :] += stiff.astype(jnp.float32)
        return carry

    lax.fori_loop(0, elems, element, 0, unroll=8)
    for copy in second:
        copy.wait()
    chunk = p_all.shape[0] // 4
    for i in range(4):
        rows = pl.ds(i * chunk, chunk)
        q_low[rows, :] = q_sum[rows, :].astype(jnp.bfloat16)
        part = lax.dot_general(
            p_all[rows, :], q_low[rows, :], (((0,), (0,)), ((), ())), preferred_element_type=jnp.float32
        )
        if i == 0:
            k_acc[...] = part
        else:
            k_acc[...] += part
    strip = modes // plan.places
    for step in range(chips):
        chip = jnp.where(kind == 1, chips - 1 - step, step)
        for cross in range(2):
            row = pl.multiple_of((chip * 2 + (core ^ cross)) * strip, strip)
            outs[2 * step + cross][...] = k_acc[pl.ds(row, strip), :].astype(jnp.bfloat16)


def final_kernel(n, where_ref, trial_ref, *refs):
    same, cross = refs[:n], refs[n : 2 * n]
    k_ref, f_ref, rows = refs[2 * n :]
    core, step = where_ref[1], where_ref[2]
    half = same[0].shape[1]
    mine = pl.ds(pl.multiple_of(core * half, half), half)
    other = pl.ds(pl.multiple_of((1 - core) * half, half), half)
    for i in range(n):

        @pl.when(step == i)
        def _():
            rows[:, mine] = same[i][...]
            rows[:, other] = cross[i][...]

    k = rows[...]
    k_ref[...] = k.astype(jnp.float32)
    f_ref[...] = jnp.dot(k, trial_ref[...], preferred_element_type=jnp.float32)


def body(plan, element_tiles, element_blocks, mode_shapes, trial_modes):
    part, place = lax.axis_index("sub"), lax.axis_index("elem")
    kind, core, chip = plan.kind(part), place % 2, place // 2
    step = jnp.where(kind == 1, plan.chips - 1 - chip, chip)
    where = jnp.stack([kind, core, step]).astype(jnp.int32)
    local, width, _ = element_tiles.shape
    depth, modes = mode_shapes.shape
    root, chips, beyond = plan.root, plan.chips, plan.beyond
    per = depth // width
    wide = modes + local // per * width
    total, elems = depth * plan.places, local * plan.places
    strip, half = modes // plan.places, modes // 2

    def send(x, pairs):
        return lax.ppermute(x, AXES, pairs)

    def kernel(fn, out, ins, scratch, limit, flops=0):
        return pl.pallas_call(
            fn,
            out_shape=out,
            in_specs=ins,
            out_specs=[VMEM] * len(out),
            scratch_shapes=scratch,
            compiler_params=pltpu.CompilerParams(vmem_limit_bytes=limit + SPARE),
            cost_estimate=pl.CostEstimate(flops=flops, bytes_accessed=0, transcendentals=0),
        )

    def array(shape, dtype=jnp.bfloat16):
        return jax.ShapeDtypeStruct(shape, dtype)

    cuts = (0, depth // 4, depth // 4 + (depth - depth // 4) // 2, depth) if plan.paired else (0, depth)
    heights = [high - low for low, high in zip(cuts[:-1], cuts[1:])]
    carrier = 1 if plan.paired else 0
    shard, *parts = kernel(
        functools.partial(pack_kernel, cuts),
        [array((depth + BELOW, wide))] + [array((n + BELOW * (i == carrier), wide)) for i, n in enumerate(heights)],
        [HBM, HBM, VMEM],
        [pltpu.VMEM((BELOW, LANES), jnp.int32), pltpu.SemaphoreType.DMA((local + 1,))],
        4 * depth * wide,
    )(mode_shapes, element_tiles, element_blocks.T)

    got = {root: shard}
    sides = [send(x, plan.aside(beyond, f)) for x, f in zip(parts[1:], plan.flips)]
    for s in range(chips - 1, -1, -1):
        if s not in (root, beyond):
            got[s] = send(shard, plan.to_root(s))
    cut = [send(parts[0], plan.to_root(beyond))]
    cut += [send(x, plan.aside_to_root(beyond, f)) for x, f in zip(sides, plan.flips)]
    [got[beyond]] = kernel(
        functools.partial(join_kernel, cuts), [array((depth + BELOW, wide))], [VMEM] * len(cut), [], 4 * depth * wide
    )(*cut)

    p_in, spans = [], []
    for s in range(chips):
        p_in += [got[s], send(got[s], plan.swap())]
        spans += [(2 * s * depth, depth), ((2 * s + 1) * depth, depth)]

    pieces = kernel(
        functools.partial(root_kernel, plan, spans, width, modes, elems),
        [array((strip, half))] * plan.places,
        [SMEM] + [ANY] * len(p_in),
        [
            pltpu.VMEM((total, modes), jnp.bfloat16),
            pltpu.VMEM((total, wide - modes), jnp.bfloat16),
            pltpu.VMEM((plan.places * BELOW, LANES), jnp.bfloat16),
            pltpu.VMEM((plan.places * BELOW, LANES), jnp.int32),
            pltpu.SMEM((plan.places * BELOW, LANES), jnp.int32),
            pltpu.VMEM((total, half), jnp.float32),
            pltpu.VMEM((total, half), jnp.bfloat16),
            pltpu.VMEM((modes, half), jnp.float32),
            pltpu.SemaphoreType.DMA((4 * len(p_in) + 1,)),
        ],
        total * (wide + 3 * half) * 2 + 8 * modes * half,
        2 * elems * width * width * half + 2 * total * modes * half,
    )(where, *p_in)
    same = [pieces[2 * s] if s == root else send(pieces[2 * s], plan.from_root(s, 0)) for s in range(chips)]
    cross = [send(pieces[2 * s + 1], plan.from_root(s, 1)) for s in range(chips)]
    return kernel(
        functools.partial(final_kernel, chips),
        [array((strip, modes), jnp.float32), array((strip, trial_modes.shape[1]), jnp.float32)],
        [SMEM] + [VMEM] * (2 * chips + 1),
        [pltpu.VMEM((strip, modes), jnp.bfloat16)],
        4 << 20,
    )(where, trial_modes, *same, *cross)


def solution(mesh):
    plan = Plan(mesh)
    in_specs = (
        P(AXES, None, None),
        P(AXES, None),
        P(AXES, None),
        P("sub", None),
    )
    out_specs = (P(AXES, None), P(AXES, None))

    def step(*args):
        return body(plan, *args)

    return jax.shard_map(step, mesh=mesh, in_specs=in_specs, out_specs=out_specs, check_vma=False)
```

```python
import functools

import jax
import jax.numpy as jnp
from jax import lax
from jax.experimental import pallas as pl
from jax.experimental.pallas import tpu as pltpu
from jax.sharding import PartitionSpec as P


AXES = ("sub", "elem")
LANES, BELOW = 128, 8
FLIPS = (1, 2, 1, 2)
CHUNKS = len(FLIPS)
SPARE = 2 << 20
SMEM = pl.BlockSpec(memory_space=pltpu.SMEM)
VMEM = pl.BlockSpec(memory_space=pltpu.VMEM)
ANY = pl.BlockSpec(memory_space=pl.ANY)
HBM = pl.BlockSpec(memory_space=pltpu.HBM)


class Plan:
    def __init__(self, mesh):
        self.parts, self.places = mesh.shape["sub"], mesh.shape["elem"]
        self.chips = self.places // 2
        self.root = self.chips // 2 - 1
        self.beyond = self.root + 1
        self.paired = self.parts % 4 == 0

    def kind(self, part):
        return (part ^ (part >> 1)) & 1 if self.paired else part * 0

    def device(self, part, step, core):
        chip = self.chips - 1 - step if self.kind(part) else step
        return part * self.places + chip * 2 + core

    def beside(self, part, step, core, flip):
        return self.device(part, step, core) + ((part ^ flip) - part) * self.places

    def pairs(self, route):
        return [route(part, core) for part in range(self.parts) for core in range(2)]

    def to_root(self, step):
        return self.pairs(lambda p, c: (self.device(p, step, c), self.device(p, self.root, c)))

    def aside(self, step, flip):
        return self.pairs(lambda p, c: (self.device(p, step, c), self.beside(p, step, c, flip)))

    def aside_to_root(self, step, flip):
        return self.pairs(lambda p, c: (self.beside(p, step, c, flip), self.device(p, self.root, c)))

    def swap(self):
        return self.pairs(lambda p, c: (self.device(p, self.root, c), self.device(p, self.root, 1 - c)))

    def from_root(self, step, cross):
        return self.pairs(lambda p, c: (self.device(p, self.root, c), self.device(p, step, c ^ cross)))


def tiles_kernel(t_ref, b_ref, out_ref, low_ref):
    local, width, _ = t_ref.shape
    for t in range(local):
        out_ref[t * width : (t + 1) * width, :] = t_ref[t]
    low_ref[...] = jnp.zeros_like(low_ref)
    low_ref[: b_ref.shape[0], :local] = b_ref[...]
    out_ref[local * width :, :] = low_ref[...].astype(jnp.float32).astype(out_ref.dtype)


def join_kernel(*refs):
    parts, all_ref = refs[:-1], refs[-1]
    row = 0
    for part in parts:
        all_ref[row : row + part.shape[0], :] = part[...]
        row += part.shape[0]


def root_kernel(plan, spans, width, modes, elems, where_ref, *refs):
    chips, n, half, below = plan.chips, len(refs) - 2 * plan.chips - 9, modes // 2, BELOW
    p_in, outs = refs[:n], refs[n : n + 2 * chips]
    p_all, t_all, low_idx, vec_idx, idx, q_sum, q_low, k_acc, sems = refs[n + 2 * chips :]
    kind, core = where_ref[0], where_ref[1]
    depth, local = p_all.shape[0] // plan.places, elems // plan.places
    per = depth // width
    mine = pl.ds(pl.multiple_of(core * half, half), half)
    rest = pl.ds(pl.multiple_of((1 - core) * half, half), half)

    first, second, numbers = [], [], []

    def copy(src, to):
        at = len(first) + len(second) + len(numbers)
        return pltpu.make_async_copy(src, to, sems.at[at])

    for slot, (p_at, t_at, low) in enumerate(spans):
        p_ref, t_ref = p_in[p_at], p_in[t_at]
        to = pl.ds(slot * depth, depth)
        numbers.append(
            copy(t_ref.at[pl.ds(low + local * width, below), :], low_idx.at[pl.ds(slot * below, below), :])
        )
        for j in range(local // per):
            block = t_ref.at[pl.ds(low + j * depth, depth), :]
            first.append(copy(block, t_all.at[to, pl.ds(j * width, width)]))
        first.append(copy(p_ref.at[:, mine], p_all.at[to, mine]))
        second.append(copy(p_ref.at[:, rest], p_all.at[to, rest]))
    for c in numbers + first + second:
        c.start()
    for c in numbers:
        c.wait()
    vec_idx[...] = low_idx[...].astype(jnp.float32).astype(jnp.int32)
    to_smem = copy(vec_idx, idx)
    to_smem.start()
    q_sum[...] = jnp.zeros_like(q_sum)
    to_smem.wait()
    for c in first:
        c.wait()

    def row_of(block):
        place, b = block // per, block % per
        chip, other = place // 2, (place % 2) ^ core
        step = jnp.where(kind == 1, chips - 1 - chip, chip)
        return pl.ds(pl.multiple_of(((step * 2 + other) * per + b) * width, width), width)

    def element(e, carry):
        slot, t = e // local, e % local
        tile = t_all[
            pl.ds(pl.multiple_of(slot * depth + t % per * width, width), width),
            pl.ds(pl.multiple_of(t // per * width, width), width),
        ]
        r, c = idx[slot * below, t], idx[slot * below + 1, t]
        stiff = jnp.dot(tile, p_all[row_of(c), mine], preferred_element_type=jnp.float32).astype(jnp.bfloat16)
        q_sum[row_of(r), :] += stiff.astype(jnp.float32)
        return carry

    lax.fori_loop(0, elems, element, 0, unroll=64)
    for c in second:
        c.wait()
    chunk = p_all.shape[0] // 4
    for i in range(4):
        rows = pl.ds(i * chunk, chunk)
        q_low[rows, :] = q_sum[rows, :].astype(jnp.bfloat16)
        part = lax.dot_general(
            p_all[rows, :], q_low[rows, :], (((0,), (0,)), ((), ())), preferred_element_type=jnp.float32
        )
        if i == 0:
            k_acc[...] = part
        else:
            k_acc[...] += part
    strip = modes // plan.places
    for step in range(chips):
        chip = jnp.where(kind == 1, chips - 1 - step, step)
        for cross in range(2):
            row = pl.multiple_of((chip * 2 + (core ^ cross)) * strip, strip)
            outs[2 * step + cross][...] = k_acc[pl.ds(row, strip), :].astype(jnp.bfloat16)


def final_kernel(n, where_ref, trial_ref, *refs):
    same, cross = refs[:n], refs[n : 2 * n]
    k_ref, f_ref, rows = refs[2 * n :]
    core, step = where_ref[1], where_ref[2]
    half = same[0].shape[1]
    mine = pl.ds(pl.multiple_of(core * half, half), half)
    other = pl.ds(pl.multiple_of((1 - core) * half, half), half)
    for i in range(n):

        @pl.when(step == i)
        def _():
            rows[:, mine] = same[i][...]
            rows[:, other] = cross[i][...]

    k = rows[...]
    k_ref[...] = k.astype(jnp.float32)
    f_ref[...] = jnp.dot(k, trial_ref[...], preferred_element_type=jnp.float32)


def body(plan, element_tiles, element_blocks, mode_shapes, trial_modes):
    part, place = lax.axis_index("sub"), lax.axis_index("elem")
    kind, core, chip = plan.kind(part), place % 2, place // 2
    step = jnp.where(kind == 1, plan.chips - 1 - chip, chip)
    where = jnp.stack([kind, core, step]).astype(jnp.int32)
    local, width, _ = element_tiles.shape
    depth, modes = mode_shapes.shape
    root, chips, beyond = plan.root, plan.chips, plan.beyond
    per = depth // width
    wide = modes + local // per * width
    total, elems = depth * plan.places, local * plan.places
    strip, half = modes // plan.places, modes // 2

    def send(x, pairs):
        return lax.ppermute(x, AXES, pairs)

    def kernel(fn, out, ins, scratch, limit, flops=0):
        return pl.pallas_call(
            fn,
            out_shape=out,
            in_specs=ins,
            out_specs=[VMEM] * len(out),
            scratch_shapes=scratch,
            compiler_params=pltpu.CompilerParams(vmem_limit_bytes=limit + SPARE),
            cost_estimate=pl.CostEstimate(flops=flops, bytes_accessed=0, transcendentals=0),
        )

    def array(shape, dtype=jnp.bfloat16):
        return jax.ShapeDtypeStruct(shape, dtype)

    def joined(parts):
        rows, columns = sum(x.shape[0] for x in parts), parts[0].shape[1]
        [whole] = kernel(join_kernel, [array((rows, columns))], [VMEM] * len(parts), [], 6 * rows * columns)(*parts)
        return whole

    chunk = depth // CHUNKS
    sides, got = [], {}
    if plan.paired:
        sides = [send(mode_shapes[i * chunk : (i + 1) * chunk], plan.aside(beyond, FLIPS[i])) for i in range(CHUNKS)]
    for s in range(chips - 1, -1, -1):
        if s != root and not (s == beyond and plan.paired):
            got[s] = [send(mode_shapes, plan.to_root(s))]
    if plan.paired:
        got[beyond] = [send(x, plan.aside_to_root(beyond, FLIPS[i])) for i, x in enumerate(sides)]
    [tiles] = kernel(
        tiles_kernel,
        [array((local * width + BELOW, width))],
        [VMEM, VMEM],
        [pltpu.VMEM((BELOW, width), jnp.int32)],
        4 * local * width * width,
    )(element_tiles, element_blocks.T)
    got[root] = [mode_shapes]
    there = {s: tiles if s == root else send(tiles, plan.to_root(s)) for s in range(chips - 1, -1, -1)}
    late = [beyond] if plan.paired else []
    early = [s for s in range(chips) if s not in late]
    p_in, place = [], {}

    def hold(x, keys):
        for core, y in enumerate((x, send(x, plan.swap()))):
            for i, key in enumerate(keys):
                place[(*key, core)] = (len(p_in), i * (local * width + BELOW))
            p_in.append(y)

    for s in range(chips):
        hold(got[s][0] if len(got[s]) == 1 else joined(got[s]), [("p", s)])
    hold(joined([there[s] for s in early]), [("t", s) for s in early])
    for s in late:
        hold(there[s], [("t", s)])
    spans = [(place["p", s, c][0], *place["t", s, c]) for s in range(chips) for c in range(2)]

    pieces = kernel(
        functools.partial(root_kernel, plan, spans, width, modes, elems),
        [array((strip, half))] * plan.places,
        [SMEM] + [ANY] * len(p_in),
        [
            pltpu.VMEM((total, modes), jnp.bfloat16),
            pltpu.VMEM((total, wide - modes), jnp.bfloat16),
            pltpu.VMEM((plan.places * BELOW, LANES), jnp.bfloat16),
            pltpu.VMEM((plan.places * BELOW, LANES), jnp.int32),
            pltpu.SMEM((plan.places * BELOW, LANES), jnp.int32),
            pltpu.VMEM((total, half), jnp.float32),
            pltpu.VMEM((total, half), jnp.bfloat16),
            pltpu.VMEM((modes, half), jnp.float32),
            pltpu.SemaphoreType.DMA((plan.places * (local // per + 3) + 1,)),
        ],
        total * (wide + 3 * half) * 2 + 4 * modes * half,
        2 * elems * width * width * half + 2 * total * modes * half,
    )(where, *p_in)
    same = [pieces[2 * s] if s == root else send(pieces[2 * s], plan.from_root(s, 0)) for s in range(chips)]
    cross = [send(pieces[2 * s + 1], plan.from_root(s, 1)) for s in range(chips)]
    return kernel(
        functools.partial(final_kernel, chips),
        [array((strip, modes), jnp.float32), array((strip, trial_modes.shape[1]), jnp.float32)],
        [SMEM] + [VMEM] * (2 * chips + 1),
        [pltpu.VMEM((strip, modes), jnp.bfloat16)],
        4 << 20,
    )(where, trial_modes, *same, *cross)


def solution(mesh):
    plan = Plan(mesh)
    in_specs = (
        P(AXES, None, None),
        P(AXES, None),
        P(AXES, None),
        P("sub", None),
    )
    out_specs = (P(AXES, None), P(AXES, None))

    def step(*args):
        return body(plan, *args)

    return jax.shard_map(step, mesh=mesh, in_specs=in_specs, out_specs=out_specs, check_vma=False)
```

```python
import functools

import jax
import jax.numpy as jnp
from jax import lax
from jax.experimental import pallas as pl
from jax.experimental.pallas import tpu as pltpu
from jax.sharding import PartitionSpec as P


AXES = ("sub", "elem")
LANES, BELOW = 128, 8
FLIPS = (1, 2, 1, 2)
CHUNKS = len(FLIPS)
SPARE = 2 << 20
SMEM = pl.BlockSpec(memory_space=pltpu.SMEM)
VMEM = pl.BlockSpec(memory_space=pltpu.VMEM)
ANY = pl.BlockSpec(memory_space=pl.ANY)
HBM = pl.BlockSpec(memory_space=pltpu.HBM)


class Plan:
    def __init__(self, mesh):
        self.parts, self.places = mesh.shape["sub"], mesh.shape["elem"]
        self.chips = self.places // 2
        self.root = self.chips // 2 - 1
        self.beyond = self.root + 1
        self.paired = self.parts % 4 == 0

    def kind(self, part):
        return (part ^ (part >> 1)) & 1 if self.paired else part * 0

    def device(self, part, step, core):
        chip = self.chips - 1 - step if self.kind(part) else step
        return part * self.places + chip * 2 + core

    def beside(self, part, step, core, flip):
        return self.device(part, step, core) + ((part ^ flip) - part) * self.places

    def pairs(self, route):
        return [route(part, core) for part in range(self.parts) for core in range(2)]

    def to_root(self, step):
        return self.pairs(lambda p, c: (self.device(p, step, c), self.device(p, self.root, c)))

    def aside(self, step, flip):
        return self.pairs(lambda p, c: (self.device(p, step, c), self.beside(p, step, c, flip)))

    def aside_to_root(self, step, flip):
        return self.pairs(lambda p, c: (self.beside(p, step, c, flip), self.device(p, self.root, c)))

    def swap(self):
        return self.pairs(lambda p, c: (self.device(p, self.root, c), self.device(p, self.root, 1 - c)))

    def from_root(self, step, cross):
        return self.pairs(lambda p, c: (self.device(p, self.root, c), self.device(p, step, c ^ cross)))


def tiles_kernel(t_ref, b_ref, out_ref, low_ref):
    local, width, _ = t_ref.shape
    for t in range(local):
        out_ref[t * width : (t + 1) * width, :] = t_ref[t]
    low_ref[...] = jnp.zeros_like(low_ref)
    low_ref[: b_ref.shape[0], :local] = b_ref[...]
    out_ref[local * width :, :] = low_ref[...].astype(jnp.float32).astype(out_ref.dtype)


def join_kernel(*refs):
    parts, all_ref = refs[:-1], refs[-1]
    row = 0
    for part in parts:
        all_ref[row : row + part.shape[0], :] = part[...]
        row += part.shape[0]


def root_kernel(plan, spans, width, modes, elems, where_ref, *refs):
    chips, n, half, below = plan.chips, len(refs) - 2 * plan.chips - 9, modes // 2, BELOW
    p_in, outs = refs[:n], refs[n : n + 2 * chips]
    p_all, t_all, low_idx, vec_idx, idx, q_sum, q_low, k_acc, sems = refs[n + 2 * chips :]
    kind, core = where_ref[0], where_ref[1]
    depth, local = p_all.shape[0] // plan.places, elems // plan.places
    per = depth // width
    mine = pl.ds(pl.multiple_of(core * half, half), half)
    rest = pl.ds(pl.multiple_of((1 - core) * half, half), half)

    first, second, numbers = [], [], []

    def copy(src, to):
        at = len(first) + len(second) + len(numbers)
        return pltpu.make_async_copy(src, to, sems.at[at])

    for slot, (p_at, t_at, low) in enumerate(spans):
        p_ref, t_ref = p_in[p_at], p_in[t_at]
        to = pl.ds(slot * depth, depth)
        numbers.append(
            copy(t_ref.at[pl.ds(low + local * width, below), :], low_idx.at[pl.ds(slot * below, below), :])
        )
        for j in range(local // per):
            block = t_ref.at[pl.ds(low + j * depth, depth), :]
            first.append(copy(block, t_all.at[to, pl.ds(j * width, width)]))
        first.append(copy(p_ref.at[:, mine], p_all.at[to, mine]))
        second.append(copy(p_ref.at[:, rest], p_all.at[to, rest]))
    for c in numbers + first + second:
        c.start()
    for c in numbers:
        c.wait()
    vec_idx[...] = low_idx[...].astype(jnp.float32).astype(jnp.int32)
    to_smem = copy(vec_idx, idx)
    to_smem.start()
    q_sum[...] = jnp.zeros_like(q_sum)
    to_smem.wait()
    for c in first:
        c.wait()

    def row_of(block):
        place, b = block // per, block % per
        chip, other = place // 2, (place % 2) ^ core
        step = jnp.where(kind == 1, chips - 1 - chip, chip)
        return pl.ds(pl.multiple_of(((step * 2 + other) * per + b) * width, width), width)

    def element(e, carry):
        slot, t = e // local, e % local
        tile = t_all[
            pl.ds(pl.multiple_of(slot * depth + t % per * width, width), width),
            pl.ds(pl.multiple_of(t // per * width, width), width),
        ]
        r, c = idx[slot * below, t], idx[slot * below + 1, t]
        stiff = jnp.dot(tile, p_all[row_of(c), mine], preferred_element_type=jnp.float32).astype(jnp.bfloat16)
        q_sum[row_of(r), :] += stiff.astype(jnp.float32)
        return carry

    lax.fori_loop(0, elems, element, 0, unroll=64)
    for c in second:
        c.wait()
    q_low[...] = q_sum[...].astype(jnp.bfloat16)
    k_acc[...] = lax.dot_general(
        p_all[...], q_low[...], (((0,), (0,)), ((), ())), preferred_element_type=jnp.float32
    )
    strip = modes // plan.places
    for step in range(chips):
        chip = jnp.where(kind == 1, chips - 1 - step, step)
        for cross in range(2):
            row = pl.multiple_of((chip * 2 + (core ^ cross)) * strip, strip)
            outs[2 * step + cross][...] = k_acc[pl.ds(row, strip), :].astype(jnp.bfloat16)


def final_kernel(n, where_ref, trial_ref, *refs):
    same, cross = refs[:n], refs[n : 2 * n]
    k_ref, f_ref = refs[2 * n :]
    core, step = where_ref[1], where_ref[2]
    half = same[0].shape[1]
    mine = pl.ds(pl.multiple_of(core * half, half), half)
    other = pl.ds(pl.multiple_of((1 - core) * half, half), half)
    for i in range(n):

        @pl.when(step == i)
        def _():
            own, far = same[i][...], cross[i][...]
            k_ref[:, mine] = own.astype(jnp.float32)
            k_ref[:, other] = far.astype(jnp.float32)
            f_ref[...] = jnp.dot(own, trial_ref[mine, :], preferred_element_type=jnp.float32) + jnp.dot(
                far, trial_ref[other, :], preferred_element_type=jnp.float32
            )


def body(plan, element_tiles, element_blocks, mode_shapes, trial_modes):
    part, place = lax.axis_index("sub"), lax.axis_index("elem")
    kind, core, chip = plan.kind(part), place % 2, place // 2
    step = jnp.where(kind == 1, plan.chips - 1 - chip, chip)
    where = jnp.stack([kind, core, step]).astype(jnp.int32)
    local, width, _ = element_tiles.shape
    depth, modes = mode_shapes.shape
    root, chips, beyond = plan.root, plan.chips, plan.beyond
    per = depth // width
    wide = modes + local // per * width
    total, elems = depth * plan.places, local * plan.places
    strip, half = modes // plan.places, modes // 2

    def send(x, pairs):
        return lax.ppermute(x, AXES, pairs)

    def kernel(fn, out, ins, scratch, limit, flops=0):
        return pl.pallas_call(
            fn,
            out_shape=out,
            in_specs=ins,
            out_specs=[VMEM] * len(out),
            scratch_shapes=scratch,
            compiler_params=pltpu.CompilerParams(vmem_limit_bytes=limit + SPARE),
            cost_estimate=pl.CostEstimate(flops=flops, bytes_accessed=0, transcendentals=0),
        )

    def array(shape, dtype=jnp.bfloat16):
        return jax.ShapeDtypeStruct(shape, dtype)

    def joined(parts):
        rows, columns = sum(x.shape[0] for x in parts), parts[0].shape[1]
        [whole] = kernel(join_kernel, [array((rows, columns))], [VMEM] * len(parts), [], 6 * rows * columns)(*parts)
        return whole

    chunk = depth // CHUNKS
    sides, got = [], {}
    if plan.paired:
        sides = [send(mode_shapes[i * chunk : (i + 1) * chunk], plan.aside(beyond, FLIPS[i])) for i in range(CHUNKS)]
    for s in range(chips - 1, -1, -1):
        if s != root and not (s == beyond and plan.paired):
            got[s] = [send(mode_shapes, plan.to_root(s))]
    if plan.paired:
        got[beyond] = [send(x, plan.aside_to_root(beyond, FLIPS[i])) for i, x in enumerate(sides)]
    [tiles] = kernel(
        tiles_kernel,
        [array((local * width + BELOW, width))],
        [VMEM, VMEM],
        [pltpu.VMEM((BELOW, width), jnp.int32)],
        4 * local * width * width,
    )(element_tiles, element_blocks.T)
    got[root] = [mode_shapes]
    there = {s: tiles if s == root else send(tiles, plan.to_root(s)) for s in range(chips - 1, -1, -1)}
    late = [beyond] if plan.paired else []
    early = [s for s in range(chips) if s not in late]
    p_in, place = [], {}

    def hold(x, keys):
        for core, y in enumerate((x, send(x, plan.swap()))):
            for i, key in enumerate(keys):
                place[(*key, core)] = (len(p_in), i * (local * width + BELOW))
            p_in.append(y)

    for s in range(chips):
        hold(got[s][0] if len(got[s]) == 1 else joined(got[s]), [("p", s)])
    hold(joined([there[s] for s in early]), [("t", s) for s in early])
    for s in late:
        hold(there[s], [("t", s)])
    spans = [(place["p", s, c][0], *place["t", s, c]) for s in range(chips) for c in range(2)]

    pieces = kernel(
        functools.partial(root_kernel, plan, spans, width, modes, elems),
        [array((strip, half))] * plan.places,
        [SMEM] + [ANY] * len(p_in),
        [
            pltpu.VMEM((total, modes), jnp.bfloat16),
            pltpu.VMEM((total, wide - modes), jnp.bfloat16),
            pltpu.VMEM((plan.places * BELOW, LANES), jnp.bfloat16),
            pltpu.VMEM((plan.places * BELOW, LANES), jnp.int32),
            pltpu.SMEM((plan.places * BELOW, LANES), jnp.int32),
            pltpu.VMEM((total, half), jnp.float32),
            pltpu.VMEM((total, half), jnp.bfloat16),
            pltpu.VMEM((modes, half), jnp.float32),
            pltpu.SemaphoreType.DMA((plan.places * (local // per + 3) + 1,)),
        ],
        total * (wide + 3 * half) * 2 + 4 * modes * half,
        2 * elems * width * width * half + 2 * total * modes * half,
    )(where, *p_in)
    same = [pieces[2 * s] if s == root else send(pieces[2 * s], plan.from_root(s, 0)) for s in range(chips)]
    cross = [send(pieces[2 * s + 1], plan.from_root(s, 1)) for s in range(chips)]
    return kernel(
        functools.partial(final_kernel, chips),
        [array((strip, modes), jnp.float32), array((strip, trial_modes.shape[1]), jnp.float32)],
        [SMEM] + [VMEM] * (2 * chips + 1),
        [],
        4 << 20,
    )(where, trial_modes, *same, *cross)


def solution(mesh):
    plan = Plan(mesh)
    in_specs = (
        P(AXES, None, None),
        P(AXES, None),
        P(AXES, None),
        P("sub", None),
    )
    out_specs = (P(AXES, None), P(AXES, None))

    def step(*args):
        return body(plan, *args)

    return jax.shard_map(step, mesh=mesh, in_specs=in_specs, out_specs=out_specs, check_vma=False)
```
